768 devices in a mesh: rep: 48 (over y_lo, z, core), fsdp: 16 (over x, y_hi).
Axes of the slice: x: 4, y: 8 (y_hi: 4, y_lo: 2; y = y_hi * 2 + y_lo), z: 12, core: 2. Of those that a mesh axis runs over, the one named last changes fastest.
Arguments:
- tokens: bfloat16 [48, 2048, 8192], P('rep', 'fsdp'), may hold values from -6 to 6
- norm_gain: bfloat16 [8192], replicated, may hold values from 0.25 to 1.75
- inner_weight: bfloat16 [48, 8192, 512], P('rep', 'fsdp'), may hold values from -0.0625 to 0.0625
- cotangent: bfloat16 [48, 2048, 512], P('rep', 'fsdp'), may hold values from -6 to 6
- fragment: bfloat16 [48, 8192, 512], P('rep', 'fsdp'), may hold values from -6 to 6
- outer_param: float32 [8192, 512], P('fsdp'), may hold values from -6 to 6
- momentum: bfloat16 [8192, 512], P('fsdp'), may hold values from -3 to 3
- lag: int32 [48], P('rep'), may hold values from 0 to 7, as said below
- threshold: int32 [1], replicated, may hold values from 1 to 6
Outputs:
- inner_grad: bfloat16 [48, 8192, 512], P('rep', 'fsdp')
- mixed: bfloat16 [48, 8192, 512], P('rep', 'fsdp')
- new_momentum: bfloat16 [8192, 512], P('fsdp')
The draws below stay inside these ranges and needn't reach their ends.
Inputs may be any that keep to these rules, and one draw needn't show every extreme that they name: At least one replica has lag 0.
All inputs are finite; a program needn't handle non-finite values.
Results may differ from the reference program's by a relative error of at most 0.006.
Values may be sent and summed in bfloat16 or wider, within the bound.
A program may use at most 64 MiB of HBM per device.

```python
import math
import jax
import jax.numpy as jnp
from jax import lax

D = 8192
KVW = 512
TOKF = 2048
REPLICAS = 48


def draw_lag(key, part):
    first, second = jax.random.split(jax.random.fold_in(key, 11))
    values = jax.random.randint(first, (REPLICAS,), 0, 8, dtype=jnp.int32)
    spot = jax.random.randint(second, (), 0, REPLICAS, dtype=jnp.int32)
    return jnp.where(jnp.arange(REPLICAS, dtype=jnp.int32) == spot, 0, values).astype(jnp.int32)


def shard_levels(rng, shape, shards, least, largest):
    def one(dim, shards_of):
        draws = jax.random.uniform(jax.random.fold_in(jax.random.fold_in(rng, 6), dim), (shards_of,), jnp.float32, least / len(shards), largest / len(shards))
        return jnp.repeat(jnp.exp(draws), shape[dim] // shards_of).reshape((-1,) + (1,) * (len(shape) - dim - 1))

    factor_of = one(*shards[0])
    for cut in shards[1:]:
        factor_of = factor_of * one(*cut)
    return factor_of


def normal_values(own_key, dims, width, reach, shards=(), kind=jnp.bfloat16):
    array = jax.random.normal(own_key, dims, jnp.float32) * width
    if len(shards) > 0:
        array = shard_levels(own_key, dims, shards, -0.22, 0.18) * array
    return jnp.clip(array, min=-reach, max=reach).astype(kind)


def setup_inputs(seed: int = 0) -> dict:
    splits = jax.random.split(jax.random.key(seed), 10)
    tokens = normal_values(splits[0], (REPLICAS, TOKF, D), 1.0, 6.0, ((0, 48), (1, 16)))
    norm_gain = jnp.clip(1.0 + 0.15 * jax.random.normal(splits[1], (D,), jnp.float32), 0.25, 1.75).astype(jnp.bfloat16)
    inner_weight = normal_values(splits[2], (REPLICAS, D, KVW), D ** -0.5, 0.0625, ((0, 48), (1, 16)))
    cotangent = normal_values(splits[3], (REPLICAS, TOKF, KVW), 1.0, 6.0, ((0, 48), (1, 16)))
    fragment = normal_values(splits[4], (REPLICAS, D, KVW), 1.0, 6.0, ((0, 48), (1, 16)))
    outer_param = normal_values(splits[5], (D, KVW), 1.0, 6.0, ((0, 16),), jnp.float32)
    momentum = normal_values(splits[6], (D, KVW), 0.5, 3.0, ((0, 16),))
    lag = draw_lag(jax.random.fold_in(splits[9], 71), 0)
    threshold = jax.random.randint(splits[8], (1,), 1, 7).astype(jnp.int32)
    return dict(tokens=tokens, norm_gain=norm_gain, inner_weight=inner_weight, cotangent=cotangent, fragment=fragment, outer_param=outer_param, momentum=momentum, lag=lag, threshold=threshold)


EPS = 1e-05
MU = 0.9
OUTER_LR = 0.7
ALPHA = 0.5

def inner_step(norm_gain, operands):
    hidden, weight, cotangent = operands
    values = hidden.astype(jnp.float32)
    normed = (values * lax.rsqrt(lax.optimization_barrier(jnp.mean(values * values, axis=1, keepdims=True)) + EPS) * norm_gain.astype(jnp.float32)).astype(jnp.bfloat16)
    key_rows = jnp.dot(normed, weight, preferred_element_type=jnp.float32)
    sigmoid_keys = jax.nn.sigmoid(key_rows)
    dkeys = (cotangent.astype(jnp.float32) * sigmoid_keys * (1.0 + key_rows * (1.0 - sigmoid_keys))).astype(jnp.bfloat16)
    gradient = lax.dot_general(normed, dkeys, (((0,), (0,)), ((), ())), preferred_element_type=jnp.float32)
    return (gradient * (1.0 / math.sqrt(hidden.shape[0]))).astype(jnp.bfloat16)

def reference(tokens, norm_gain, inner_weight, cotangent, fragment, outer_param, momentum, lag, threshold):
    inner_grad = lax.map(lambda operands: inner_step(norm_gain, operands), (tokens, inner_weight, cotangent))
    included = (lag <= threshold[0]).astype(jnp.float32)
    count = jnp.sum(included)
    scale = 1.0 / count

    def accumulate(total, operands):
        replica_frag, flag = operands
        return (total + flag * (outer_param - replica_frag.astype(jnp.float32)), None)
    total, _ = lax.scan(accumulate, jnp.zeros(outer_param.shape, jnp.float32), (fragment, included))
    average = total * scale
    moment = MU * momentum.astype(jnp.float32) + average
    new_outer = outer_param - OUTER_LR * (average + MU * moment)
    mixed = (ALPHA * fragment.astype(jnp.float32) + (1.0 - ALPHA) * new_outer[None]).astype(jnp.bfloat16)
    return (inner_grad, mixed, moment.astype(jnp.bfloat16))
```

```python
import math

import jax
import jax.numpy as jnp
from jax import lax
from jax.experimental import pallas as pl
from jax.experimental.pallas import tpu as pltpu
from jax.sharding import PartitionSpec as P

EPS = 1e-05
MU = 0.9
OUTER_LR = 0.7
ALPHA = 0.5

NX, NY, NZ = 4, 4, 12
TOK = 128
FB = 512
KV = 512
NK = 4
KC = KV // NK
SHARE = 96
PACK = SHARE + 16
HALF = 1024
F32, BF16 = jnp.float32, jnp.bfloat16
MESH = pl.DeviceIdType.MESH


def kernel(
    tokens, gain, weight, cotangent, fragment, outer, momentum, lag, threshold,
    grad_out, mixed_out, mom_out,
    tokv, tokr, rst_s, rst_r, nrm, nrt, wown, wq, cotv,
    rs_own, rs_s, rs_r, ry_s, ry_r, dk, g_own, g_s, g_r, gout,
    fragv, outv, momv, msk, f1r, zs, zr, ys, yr, avg, mixv, momo,
    local_sem, tok_ss, tok_rs, rst_ss, rst_rs, w_ss, w_rs,
    rx_ss, rx_rs, ry_ss, ry_rs, ay_ss, ay_rs, ax_ss, ax_rs, gr_ss, gr_rs,
    f_ss, f_rs, z_ss, z_rs, az_ss, az_rs, out_sem,
):
    rep, fs = lax.axis_index("rep"), lax.axis_index("fsdp")
    core, z, ylo = lax.rem(rep, 2), lax.rem(rep // 2, NZ), rep // (2 * NZ)
    x, y = fs // NY, lax.rem(fs, NY)
    s = 1 - 2 * lax.rem(y + core, 2)
    yp = lax.rem(y + s + NY, NY)
    yq = lax.rem(y - s + NY, NY)
    yo = lax.rem(y + 2, NY)

    def at(i, yy):
        return (rep, lax.rem(x + i + NX, NX) * NY + yy)

    def at_z(i):
        return (ylo * 2 * NZ + lax.rem(z + i, NZ) * 2 + core, fs)

    other_core = (ylo * 2 * NZ + z * 2 + (1 - core), fs)
    other_ylo = ((1 - ylo) * 2 * NZ + z * 2 + core, fs)
    group = [(i, e) for e in (1, 0) for i in (2, 1, 3, 0) if (i, e) != (0, 0)]

    def remote(src, dst, ss, rs, device):
        return pltpu.make_async_remote_copy(
            src_ref=src, dst_ref=dst, send_sem=ss, recv_sem=rs, device_id=device, device_id_type=MESH
        )

    barrier = pltpu.get_barrier_semaphore()
    peers = [at(i, yp if e else y) for i, e in group] + [at(0, yq), other_core, other_ylo]
    peers += [at_z(i) for i in range(1, NZ)]
    for peer in peers:
        pl.semaphore_signal(barrier, inc=1, device_id=peer, device_id_type=MESH)

    tok_in = [
        pltpu.make_async_copy(tokens.at[0, :, pl.ds(b * FB, FB)], tokv.at[b], local_sem.at[b])
        for b in range(NX * NY)
    ]
    w_in = [
        pltpu.make_async_copy(weight.at[0, :, pl.ds(k * KC, KC)], wown.at[k], local_sem.at[16 + k])
        for k in range(NK)
    ]
    frag_in = [
        pltpu.make_async_copy(fragment.at[0, :, pl.ds(c * 128, 128)], fragv.at[c], local_sem.at[20 + c])
        for c in range(4)
    ]
    out_in = [
        pltpu.make_async_copy(outer.at[:, pl.ds(c * 128, 128)], outv.at[c], local_sem.at[24 + c])
        for c in range(4)
    ]
    mom_in = [
        pltpu.make_async_copy(momentum.at[:, pl.ds(c * 128, 128)], momv.at[c], local_sem.at[28 + c])
        for c in range(4)
    ]
    cot_in = pltpu.make_async_copy(cotangent.at[0], cotv, local_sem.at[32])
    loads = tok_in + w_in + frag_in + out_in + [cot_in] + mom_in
    for copy in loads:
        copy.start()
    for copy in tok_in + w_in:
        copy.wait()
    pl.semaphore_wait(barrier, len(peers))

    tok_copies = {}
    for n, (i, e) in enumerate(group):
        yd = yp if e else y
        cross = yo if e else yq
        xd = lax.rem(x + i, NX)
        for f, yf in enumerate((yd, cross)):
            copy = remote(
                tokv.at[xd * NY + yf], tokr.at[f, i * 2 + e],
                tok_ss.at[2 * n + f], tok_rs.at[2 * n + f], at(i, yd),
            )
            copy.start()
            tok_copies[i, e, f] = copy
    w_copies = [
        remote(wown.at[k], wq.at[k], w_ss.at[k], w_rs.at[k], at(0, yq)) for k in range(NK)
    ]
    for copy in w_copies:
        copy.start()

    flag = jnp.where(lag[0] <= threshold[0], 1.0, 0.0).astype(F32)
    for copy in frag_in:
        copy.wait()
    for h in range(2):
        part = fragv[(1 - core) * 2 + h].astype(F32) * flag
        msk[pl.ds(h * 512, 512), :] = part.astype(BF16)
    msk[pl.ds(HALF, 16), :] = jnp.full((16, 128), flag, F32).astype(BF16)
    f1_copy = remote(msk, f1r, f_ss.at[0], f_rs.at[0], other_core)
    f1_copy.start()

    def square(b, total):
        v = tokv[b].astype(F32)
        v = v * v
        return total + (v[:, 0:128] + v[:, 128:256]) + (v[:, 256:384] + v[:, 384:512])

    sums = lax.fori_loop(0, NX * NY, square, jnp.zeros((TOK, 128), F32))
    scale_own = lax.rsqrt(jnp.sum(sums, axis=1, keepdims=True) * (1.0 / (NX * NY * FB)) + EPS)
    rst_s[...] = jnp.broadcast_to(scale_own, (TOK, 128)).T[0:8, :]
    rst_copies = {}
    for n, (i, e) in enumerate(group):
        copy = remote(
            rst_s, rst_r.at[i * 2 + e], rst_ss.at[n], rst_rs.at[n], at(i, yp if e else y)
        )
        copy.start()
        rst_copies[i, e] = copy

    gains = [gain[pl.ds(x * NY + yy, 1), :] for yy in (y, yq)]

    def normalise(i, e):
        slot = i * 2 + e
        if slot == 0:
            scale = scale_own
        else:
            rst_copies[i, e].wait_recv()
            scale = jnp.broadcast_to(rst_r[slot, 0:1, :], (TOK, 128)).T[:, 0:1]
        for f in range(2):
            if slot == 0:
                raw = tokv[x * NY + (yq if f else y)]
            else:
                tok_copies[i, e, f].wait_recv()
                raw = tokr[f, slot]
            v = raw.astype(F32) * scale * gains[f]
            nrm[f, pl.ds(slot * TOK, TOK), :] = v.astype(BF16)
            nrt[f, :, pl.ds(slot * TOK, TOK)] = v.T.astype(BF16)

    normalise(0, 0)

    f1_copy.wait_recv()
    for copy in out_in:
        copy.wait()
    both = f1r[pl.ds(HALF, 16), :].astype(F32) + flag
    row = both[0:1, :]
    for j in range(NZ):
        for r in range(0, SHARE, 32):
            first = j * SHARE + r
            if first < HALF:
                block, at_row = core * 2 + first // 512, first % 512
                mine = fragv[block, pl.ds(at_row, 32), :].astype(F32) * flag
                theirs = f1r[pl.ds(first, 32), :].astype(F32)
                value = row * outv[block, pl.ds(at_row, 32), :] - (mine + theirs)
            else:
                value = jnp.zeros((32, 128), F32)
            zs[j, pl.ds(r, 32), :] = value.astype(BF16)
        zs[j, pl.ds(SHARE, 16), :] = both.astype(BF16)
    z_copies = [
        remote(zs.at[lax.rem(z + i, NZ)], zr.at[i], z_ss.at[i], z_rs.at[i], at_z(i))
        for i in (6, 5, 7, 4, 8, 3, 9, 2, 10, 1, 11)
    ]
    for copy in z_copies:
        copy.start()

    for i, e in ((1, 0), (3, 0), (2, 0), (0, 1), (1, 1), (3, 1), (2, 1)):
        normalise(i, e)

    rx, ry, ay, ax, gr = {}, {}, {}, {}, {}

    def keys_partial(k):
        w_copies[k].wait_recv()
        for i in (2, 1, 3, 0):
            rows = pl.ds(i * 2 * TOK, 2 * TOK)
            part = jnp.dot(nrm[0, rows, :], wown[k], preferred_element_type=F32)
            part += jnp.dot(nrm[1, rows, :], wq[k], preferred_element_type=F32)
            if i == 0:
                rs_own[k] = part
            else:
                rs_s[k, i] = part.astype(BF16)
                n = k * NX + i
                rx[k, i] = remote(rs_s.at[k, i], rs_r.at[k, i], rx_ss.at[n], rx_rs.at[n], at(-i, y))
                rx[k, i].start()

    def sum_x(k):
        for i in (1, 3, 2):
            rx[k, i].wait_recv()
        total = rs_own[k]
        for i in (1, 2, 3):
            total += rs_r[k, i].astype(F32)
        rs_own[k] = total
        ry_s[k] = total[TOK:, :].astype(BF16)
        ry[k] = remote(ry_s.at[k], ry_r.at[k], ry_ss.at[k], ry_rs.at[k], at(0, yp))
        ry[k].start()

    def send_x(k, e):
        for i in (2, 1, 3):
            n = (k * NX + i) * 2 + e
            ax[k, i, e] = remote(
                dk.at[k, pl.ds(e * TOK, TOK)], dk.at[k, pl.ds((i * 2 + e) * TOK, TOK)],
                ax_ss.at[n], ax_rs.at[n], at(i, y),
            )
            ax[k, i, e].start()

    def dkeys(k):
        ry[k].wait_recv()
        keys = rs_own[k, 0:TOK, :] + ry_r[k].astype(F32)
        sig = jax.nn.sigmoid(keys)
        cot = cotv[:, pl.ds(k * KC, KC)].astype(F32)
        dk[k, 0:TOK, :] = (cot * sig * (1.0 + keys * (1.0 - sig))).astype(BF16)
        ay[k] = remote(
            dk.at[k, pl.ds(0, TOK)], dk.at[k, pl.ds(TOK, TOK)], ay_ss.at[k], ay_rs.at[k], at(0, yp)
        )
        ay[k].start()
        send_x(k, 0)

    def forward(k):
        ay[k].wait_recv()
        send_x(k, 1)

    def gradient(k):
        for e in range(2):
            for i in (1, 3, 2):
                ax[k, i, e].wait_recv()
        g_s[k] = jnp.dot(nrt[1], dk[k], preferred_element_type=F32).astype(BF16)
        gr[k] = remote(g_s.at[k], g_r.at[k], gr_ss.at[k], gr_rs.at[k], at(0, yq))
        gr[k].start()
        g_own[k] = jnp.dot(nrt[0], dk[k], preferred_element_type=F32)

    outs = []

    def finish(k):
        gr[k].wait_recv()
        total = g_own[k] + g_r[k].astype(F32)
        gout[k] = (total * (1.0 / math.sqrt(NX * NY * TOK))).astype(BF16)
        copy = pltpu.make_async_copy(gout.at[k], grad_out.at[0, :, pl.ds(k * KC, KC)], out_sem.at[k])
        copy.start()
        outs.append(copy)

    y_copy = remote(ys, yr, f_ss.at[1], f_rs.at[1], other_ylo)

    def sum_z():
        total = zs[z].astype(F32)
        for copy in z_copies:
            copy.wait_recv()
        for i in range(1, NZ):
            total += zr[i].astype(F32)
        ys[...] = total
        y_copy.start()

    own_share = avg.at[core, pl.ds(pl.multiple_of(z * SHARE, SHARE), SHARE)]
    az_copies = [
        remote(own_share, own_share, az_ss.at[i], az_rs.at[i], at_z(i))
        for i in (6, 5, 7, 4, 8, 3, 9, 2, 10, 1, 11)
    ]
    core_copy = remote(avg.at[core], avg.at[core], f_ss.at[2], f_rs.at[2], other_core)

    def share_average():
        y_copy.wait_recv()
        total = ys[...] + yr[...]
        scale = 1.0 / total[SHARE : SHARE + 1, :]
        own_share[...] = (total[0:SHARE, :] * scale).astype(BF16)
        for copy in az_copies:
            copy.start()

    def gather_average():
        for copy in az_copies:
            copy.wait_recv()
        core_copy.start()

    def outer_update():
        for copy in mom_in:
            copy.wait()
        core_copy.wait_recv()
        for c in range(4):
            average = avg[c // 2, pl.ds(c % 2 * 512, 512), :].astype(F32)
            moment = MU * momv[c].astype(F32) + average
            new_outer = outv[c] - OUTER_LR * (average + MU * moment)
            mixv[c] = (ALPHA * fragv[c].astype(F32) + (1.0 - ALPHA) * new_outer).astype(BF16)
            momo[c] = moment.astype(BF16)
            for buf, out, n in ((mixv, mixed_out.at[0], 4 + c), (momo, mom_out, 8 + c)):
                copy = pltpu.make_async_copy(buf.at[c], out.at[:, pl.ds(c * 128, 128)], out_sem.at[n])
                copy.start()
                outs.append(copy)

    cot_in.wait()
    stages = [keys_partial, sum_x, dkeys, forward, gradient, finish]
    extra = {1: sum_z, 2: share_average, 5: gather_average, 6: outer_update}
    for slot in range(NK + len(stages) - 1):
        for n in reversed(range(len(stages))):
            if 0 <= slot - n < NK:
                stages[n](slot - n)
        if slot in extra:
            extra[slot]()

    for copy in outs:
        copy.wait()
    sent = list(tok_copies.values()) + w_copies + [f1_copy, y_copy, core_copy]
    sent += list(rst_copies.values()) + z_copies + az_copies
    for group_of in (rx, ry, ay, ax, gr):
        sent += list(group_of.values())
    for copy in sent:
        copy.wait_send()


def shards(
    tokens, norm_gain, inner_weight, cotangent, fragment, outer_param, momentum, lag, threshold
):
    vmem, dma = pltpu.VMEM, pltpu.SemaphoreType.DMA
    hbm = pl.BlockSpec(memory_space=pl.ANY)
    smem = pl.BlockSpec(memory_space=pltpu.SMEM)
    return pl.pallas_call(
        kernel,
        out_shape=(
            jax.ShapeDtypeStruct((1, FB, KV), BF16),
            jax.ShapeDtypeStruct((1, FB, KV), BF16),
            jax.ShapeDtypeStruct((FB, KV), BF16),
        ),
        in_specs=[hbm, pl.BlockSpec(memory_space=pltpu.VMEM), hbm, hbm, hbm, hbm, hbm, smem, smem],
        out_specs=(hbm, hbm, hbm),
        scratch_shapes=[
            vmem((16, TOK, FB), BF16),
            vmem((2, 8, TOK, FB), BF16),
            vmem((8, 128), F32),
            vmem((8, 8, 128), F32),
            vmem((2, 8 * TOK, FB), BF16),
            vmem((2, FB, 8 * TOK), BF16),
            vmem((NK, FB, KC), BF16),
            vmem((NK, FB, KC), BF16),
            vmem((TOK, KV), BF16),
            vmem((NK, 2 * TOK, KC), F32),
            vmem((NK, NX, 2 * TOK, KC), BF16),
            vmem((NK, NX, 2 * TOK, KC), BF16),
            vmem((NK, TOK, KC), BF16),
            vmem((NK, TOK, KC), BF16),
            vmem((NK, 8 * TOK, KC), BF16),
            vmem((NK, FB, KC), F32),
            vmem((NK, FB, KC), BF16),
            vmem((NK, FB, KC), BF16),
            vmem((NK, FB, KC), BF16),
            vmem((4, 512, 128), BF16),
            vmem((4, 512, 128), F32),
            vmem((4, 512, 128), BF16),
            vmem((HALF + 16, 128), BF16),
            vmem((HALF + 16, 128), BF16),
            vmem((NZ, PACK, 128), BF16),
            vmem((NZ, PACK, 128), BF16),
            vmem((PACK, 128), F32),
            vmem((PACK, 128), F32),
            vmem((2, NZ * SHARE, 128), BF16),
            vmem((4, 512, 128), BF16),
            vmem((4, 512, 128), BF16),
            dma((33,)),
            dma((14,)), dma((14,)),
            dma((7,)), dma((7,)),
            dma((NK,)), dma((NK,)),
            dma((NK * NX,)), dma((NK * NX,)),
            dma((NK,)), dma((NK,)),
            dma((NK,)), dma((NK,)),
            dma((NK * NX * 2,)), dma((NK * NX * 2,)),
            dma((NK,)), dma((NK,)),
            dma((3,)), dma((3,)),
            dma((NZ,)), dma((NZ,)),
            dma((NZ,)), dma((NZ,)),
            dma((12,)),
        ],
        compiler_params=pltpu.CompilerParams(
            collective_id=0, has_side_effects=True, vmem_limit_bytes=48 * 1024 * 1024
        ),
        name="window",
    )(
        tokens,
        norm_gain.reshape(16, FB).astype(F32),
        inner_weight,
        cotangent,
        fragment,
        outer_param,
        momentum,
        lag,
        threshold,
    )


def solution(mesh):
    placed = (
        P("rep", "fsdp", None),
        P(),
        P("rep", "fsdp", None),
        P("rep", "fsdp", None),
        P("rep", "fsdp", None),
        P("fsdp", None),
        P("fsdp", None),
        P("rep"),
        P(),
    )
    return jax.shard_map(
        shards,
        mesh=mesh,
        in_specs=placed,
        out_specs=(P("rep", "fsdp", None), P("rep", "fsdp", None), P("fsdp", None)),
        check_vma=False,
    )
```

```python
import math

import jax
import jax.numpy as jnp
from jax import lax
from jax.experimental import pallas as pl
from jax.experimental.pallas import tpu as pltpu
from jax.sharding import PartitionSpec as P

EPS = 1e-05
MU = 0.9
OUTER_LR = 0.7
ALPHA = 0.5
STARTS = (0.0, 4.3, 8.0, 13.0, 19.0)
STEP = 2.6

NX, NY, NZ = 4, 4, 12
TOK = 128
FB = 512
KV = 512
NK = 4
KC = KV // NK
SHARE = 96
PACK = SHARE + 16
HALF = 1024
F32, BF16 = jnp.float32, jnp.bfloat16
MESH = pl.DeviceIdType.MESH


def kernel(
    tokens, gain, weight, cotangent, fragment, outer, momentum, lag, threshold,
    grad_out, mixed_out, mom_out,
    tokv, tokr, rst_s, rst_r, nrm, nrt, wown, wq, cotv,
    rs_own, rs_s, rs_r, ry_s, ry_r, dk, g_own, g_s, g_r, gout,
    gainv, gainf, fragv, outv, momv, msk, f1r, zs, zr, ys, yr, avg, mixv, momo,
    local_sem, tok_ss, tok_rs, rst_ss, rst_rs, w_ss, w_rs,
    rx_ss, rx_rs, ry_ss, ry_rs, ax_ss, ax_rs, gr_ss, gr_rs,
    f_ss, f_rs, z_ss, z_rs, az_ss, az_rs, out_sem,
):
    rep, fs = lax.axis_index("rep"), lax.axis_index("fsdp")
    core, z, ylo = lax.rem(rep, 2), lax.rem(rep // 2, NZ), rep // (2 * NZ)
    x, y = fs // NY, lax.rem(fs, NY)
    s = 1 - 2 * lax.rem(y + core, 2)
    yp = lax.rem(y + s + NY, NY)
    yq = lax.rem(y - s + NY, NY)
    yo = lax.rem(y + 2, NY)

    def at(i, yy):
        return (rep, lax.rem(x + i + NX, NX) * NY + yy)

    def at_z(i):
        return (ylo * 2 * NZ + lax.rem(z + i, NZ) * 2 + core, fs)

    other_core = (ylo * 2 * NZ + z * 2 + (1 - core), fs)
    other_ylo = ((1 - ylo) * 2 * NZ + z * 2 + core, fs)
    group = [(i, e) for e in (1, 0) for i in (2, 1, 3, 0) if (i, e) != (0, 0)]

    def remote(src, dst, ss, rs, device):
        return pltpu.make_async_remote_copy(
            src_ref=src, dst_ref=dst, send_sem=ss, recv_sem=rs, device_id=device, device_id_type=MESH
        )

    barrier = pltpu.get_barrier_semaphore()
    peers = [at(i, yp if e else y) for i, e in group] + [at(0, yq), other_core, other_ylo]
    peers += [at_z(i) for i in range(1, NZ)]
    for peer in peers:
        pl.semaphore_signal(barrier, inc=1, device_id=peer, device_id_type=MESH)

    tok_in = [
        pltpu.make_async_copy(tokens.at[0, :, pl.ds(b * FB, FB)], tokv.at[b], local_sem.at[b])
        for b in range(NX * NY)
    ]
    w_in = [
        pltpu.make_async_copy(weight.at[0, :, pl.ds(k * KC, KC)], wown.at[k], local_sem.at[16 + k])
        for k in range(NK)
    ]
    frag_in = [
        pltpu.make_async_copy(fragment.at[0, :, pl.ds(c * 128, 128)], fragv.at[c], local_sem.at[20 + c])
        for c in range(4)
    ]
    out_in = [
        pltpu.make_async_copy(outer.at[:, pl.ds(c * 128, 128)], outv.at[c], local_sem.at[24 + c])
        for c in range(4)
    ]
    mom_in = [
        pltpu.make_async_copy(momentum.at[:, pl.ds(c * 128, 128)], momv.at[c], local_sem.at[28 + c])
        for c in range(4)
    ]
    cot_in = pltpu.make_async_copy(cotangent.at[0], cotv.at[0], local_sem.at[32])
    gain_in = pltpu.make_async_copy(gain, gainv, local_sem.at[33])
    loads = tok_in + w_in + frag_in + out_in + [cot_in, gain_in] + mom_in
    for copy in loads:
        copy.start()
    with jax.named_scope("load_wait"):
        for copy in tok_in + w_in:
            copy.wait()
    with jax.named_scope("barrier"):
        pl.semaphore_wait(barrier, len(peers))

    tok_copies = {}
    for n, (i, e) in enumerate(group):
        yd = yp if e else y
        cross = yo if e else yq
        xd = lax.rem(x + i, NX)
        for f, yf in enumerate((yd, cross)):
            copy = remote(
                tokv.at[xd * NY + yf], tokr.at[f, i * 2 + e],
                tok_ss.at[2 * n + f], tok_rs.at[2 * n + f], at(i, yd),
            )
            copy.start()
            tok_copies[i, e, f] = copy
    w_copies = [
        remote(wown.at[k], wq.at[k], w_ss.at[k], w_rs.at[k], at(0, yq)) for k in range(NK)
    ]
    w_copies[0].start()
    cot_in.wait()
    cot_copy = remote(cotv.at[0], cotv.at[1], f_ss.at[3], f_rs.at[3], at(0, yp))

    flag = jnp.where(lag[0] <= threshold[0], 1.0, 0.0).astype(F32)
    for copy in frag_in:
        copy.wait()
    for h in range(2):
        part = fragv[(1 - core) * 2 + h].astype(F32) * flag
        msk[pl.ds(h * 512, 512), :] = part.astype(BF16)
    msk[pl.ds(HALF, 16), :] = jnp.full((16, 128), flag, F32).astype(BF16)
    f1_copy = remote(msk, f1r, f_ss.at[0], f_rs.at[0], other_core)
    f1_copy.start()

    def square(b, total):
        v = tokv[b].astype(F32)
        v = v * v
        return total + (v[:, 0:128] + v[:, 128:256]) + (v[:, 256:384] + v[:, 384:512])

    sums = lax.fori_loop(0, NX * NY, square, jnp.zeros((TOK, 128), F32))
    scale_own = lax.rsqrt(jnp.sum(sums, axis=1, keepdims=True) * (1.0 / (NX * NY * FB)) + EPS)
    rst_s[...] = jnp.broadcast_to(scale_own, (TOK, 128)).T[0:8, :]
    rst_copies = {}
    for n, (i, e) in enumerate(group):
        copy = remote(
            rst_s, rst_r.at[i * 2 + e], rst_ss.at[n], rst_rs.at[n], at(i, yp if e else y)
        )
        copy.start()
        rst_copies[i, e] = copy

    gain_in.wait()
    gainf[...] = gainv[...].astype(F32)
    gains = [
        jnp.concatenate([gainf[pl.ds((x * NY + yy) * 4 + j, 1), :] for j in range(4)], axis=1)
        for yy in (y, yq)
    ]

    def normalise(i, e):
        slot = i * 2 + e
        if slot == 0:
            scale = scale_own
        else:
            rst_copies[i, e].wait_recv()
            scale = jnp.broadcast_to(rst_r[slot, 0:1, :], (TOK, 128)).T[:, 0:1]
        for f in range(2):
            if slot == 0:
                raw = tokv[x * NY + (yq if f else y)]
            else:
                tok_copies[i, e, f].wait_recv()
                raw = tokr[f, slot]
            v = raw.astype(F32) * scale * gains[f]
            nrm[f, pl.ds(slot * TOK, TOK), :] = v.astype(BF16)
            nrt[f, :, pl.ds(slot * TOK, TOK)] = v.T.astype(BF16)

    with jax.named_scope("norm_own"):
        normalise(0, 0)

    with jax.named_scope("f1_wait"):
        f1_copy.wait_recv()
        for copy in out_in:
            copy.wait()
    both = f1r[pl.ds(HALF, 16), :].astype(F32) + flag
    row = both[0:1, :]
    for j in range(NZ):
        for r in range(0, SHARE, 32):
            first = j * SHARE + r
            if first < HALF:
                block, at_row = core * 2 + first // 512, first % 512
                mine = fragv[block, pl.ds(at_row, 32), :].astype(F32) * flag
                theirs = f1r[pl.ds(first, 32), :].astype(F32)
                value = row * outv[block, pl.ds(at_row, 32), :] - (mine + theirs)
            else:
                value = jnp.zeros((32, 128), F32)
            zs[j, pl.ds(r, 32), :] = value.astype(BF16)
        zs[j, pl.ds(SHARE, 16), :] = both.astype(BF16)
    z_copies = [
        remote(zs.at[lax.rem(z + i, NZ)], zr.at[i], z_ss.at[i], z_rs.at[i], at_z(i))
        for i in (6, 5, 7, 4, 8, 3, 9, 2, 10, 1, 11)
    ]
    for copy in z_copies:
        copy.start()

    y_copy = remote(ys, yr, f_ss.at[1], f_rs.at[1], other_ylo)

    def sum_z():
        total = zs[z].astype(F32)
        for copy in z_copies:
            copy.wait_recv()
        for i in range(1, NZ):
            total += zr[i].astype(F32)
        ys[...] = total
        y_copy.start()

    own_share = avg.at[core, pl.ds(pl.multiple_of(z * SHARE, SHARE), SHARE)]
    az_copies = [
        remote(own_share, own_share, az_ss.at[i], az_rs.at[i], at_z(i))
        for i in (6, 5, 7, 4, 8, 3, 9, 2, 10, 1, 11)
    ]
    core_copy = remote(avg.at[core], avg.at[core], f_ss.at[2], f_rs.at[2], other_core)

    def share_average():
        y_copy.wait_recv()
        total = ys[...] + yr[...]
        scale = 1.0 / total[SHARE : SHARE + 1, :]
        own_share[...] = (total[0:SHARE, :] * scale).astype(BF16)
        for copy in az_copies:
            copy.start()

    for i, e in ((1, 0), (3, 0), (2, 0), (0, 1), (1, 1), (3, 1), (2, 1)):
        with jax.named_scope(f"norm_{i}{e}"):
            normalise(i, e)
        if (i, e) == (2, 0):
            with jax.named_scope("sum_z"):
                sum_z()
            w_copies[1].start()
        if (i, e) == (0, 1):
            w_copies[2].start()
            w_copies[3].start()
            cot_copy.start()

    rx, ry, ax, gr = {}, {}, {}, {}

    def keys_partial(k):
        w_copies[k].wait_recv()
        for i in (2, 1, 3, 0):
            rows = pl.ds(i * 2 * TOK, 2 * TOK)
            part = jnp.dot(nrm[0, rows, :], wown[k], preferred_element_type=F32)
            part += jnp.dot(nrm[1, rows, :], wq[k], preferred_element_type=F32)
            if i == 0:
                rs_own[k] = part
            else:
                rs_s[k, i] = part.astype(BF16)
                n = k * NX + i
                rx[k, i] = remote(rs_s.at[k, i], rs_r.at[k, i], rx_ss.at[n], rx_rs.at[n], at(-i, y))
                rx[k, i].start()

    def sum_x(k):
        for i in (1, 3, 2):
            rx[k, i].wait_recv()
        total = rs_own[k]
        for i in (1, 2, 3):
            total += rs_r[k, i].astype(F32)
        rs_own[k] = total
        ry_s[k, 0:TOK, :] = total[TOK:, :].astype(BF16)
        ry_s[k, TOK:, :] = total[0:TOK, :].astype(BF16)
        ry[k] = remote(ry_s.at[k], ry_r.at[k], ry_ss.at[k], ry_rs.at[k], at(0, yp))
        ry[k].start()

    def dkeys(k):
        if k == 0:
            cot_copy.wait_recv()
        ry[k].wait_recv()
        keys = rs_own[k] + ry_r[k].astype(F32)
        sig = jax.nn.sigmoid(keys)
        cot = cotv[:, :, pl.ds(k * KC, KC)].astype(F32).reshape(2 * TOK, KC)
        dk[k, 0 : 2 * TOK, :] = (cot * sig * (1.0 + keys * (1.0 - sig))).astype(BF16)
        for i in (2, 1, 3):
            n = k * NX + i
            ax[k, i] = remote(
                dk.at[k, pl.ds(0, 2 * TOK)], dk.at[k, pl.ds(i * 2 * TOK, 2 * TOK)],
                ax_ss.at[n], ax_rs.at[n], at(i, y),
            )
            ax[k, i].start()

    def gradient(k):
        for i in (1, 3, 2):
            ax[k, i].wait_recv()
        g_s[k] = jnp.dot(nrt[1], dk[k], preferred_element_type=F32).astype(BF16)
        gr[k] = remote(g_s.at[k], g_r.at[k], gr_ss.at[k], gr_rs.at[k], at(0, yq))
        gr[k].start()
        g_own[k] = jnp.dot(nrt[0], dk[k], preferred_element_type=F32)

    outs = []

    def finish(k):
        gr[k].wait_recv()
        total = g_own[k] + g_r[k].astype(F32)
        gout[k] = (total * (1.0 / math.sqrt(NX * NY * TOK))).astype(BF16)
        copy = pltpu.make_async_copy(gout.at[k], grad_out.at[0, :, pl.ds(k * KC, KC)], out_sem.at[k])
        copy.start()
        outs.append(copy)

    def gather_average():
        for copy in az_copies:
            copy.wait_recv()
        core_copy.start()

    def outer_update():
        for copy in mom_in:
            copy.wait()
        core_copy.wait_recv()
        for c in range(4):
            average = avg[c // 2, pl.ds(c % 2 * 512, 512), :].astype(F32)
            moment = MU * momv[c].astype(F32) + average
            new_outer = outv[c] - OUTER_LR * (average + MU * moment)
            mixv[c] = (ALPHA * fragv[c].astype(F32) + (1.0 - ALPHA) * new_outer).astype(BF16)
            momo[c] = moment.astype(BF16)
            for buf, out, n in ((mixv, mixed_out.at[0], 4 + c), (momo, mom_out, 8 + c)):
                copy = pltpu.make_async_copy(buf.at[c], out.at[:, pl.ds(c * 128, 128)], out_sem.at[n])
                copy.start()
                outs.append(copy)

    stages = [keys_partial, sum_x, dkeys, gradient, finish]
    steps = [(t + k * STEP, stage, k) for stage, t in zip(stages, STARTS) for k in range(NK)]
    outer_stages = ((share_average, 4.0), (gather_average, 20.0), (outer_update, 22.0))
    steps += [(t, stage, None) for stage, t in outer_stages]
    for _, stage, k in sorted(steps, key=lambda step: step[0]):
        with jax.named_scope(f"{stage.__name__}_{k}"):
            stage() if k is None else stage(k)

    with jax.named_scope("outs"):
        for copy in outs:
            copy.wait()
    sent = list(tok_copies.values()) + w_copies + [f1_copy, y_copy, core_copy, cot_copy]
    sent += list(rst_copies.values()) + z_copies + az_copies
    for group_of in (rx, ry, ax, gr):
        sent += list(group_of.values())
    for copy in sent:
        copy.wait_send()


def put_out(grad, mixed, mom, grad_out, mixed_out, mom_out, g, m, o, sem):
    into = [pltpu.make_async_copy(a, b, sem.at[n]) for n, (a, b) in enumerate(((grad, g), (mixed, m), (mom, o)))]
    out = [
        pltpu.make_async_copy(a, b, sem.at[3 + n])
        for n, (a, b) in enumerate(((g, grad_out), (m, mixed_out), (o, mom_out)))
    ]
    for copy in into:
        copy.start()
    for first, second in zip(into, out):
        first.wait()
        second.start()
    for copy in out:
        copy.wait()


def shards(
    tokens, norm_gain, inner_weight, cotangent, fragment, outer_param, momentum, lag, threshold
):
    vmem, dma = pltpu.VMEM, pltpu.SemaphoreType.DMA
    hbm = pl.BlockSpec(memory_space=pltpu.HBM)
    anywhere = pl.BlockSpec(memory_space=pl.ANY)
    smem = pl.BlockSpec(memory_space=pltpu.SMEM)
    shapes = (
        jax.ShapeDtypeStruct((1, FB, KV), BF16),
        jax.ShapeDtypeStruct((1, FB, KV), BF16),
        jax.ShapeDtypeStruct((FB, KV), BF16),
    )
    results = pl.pallas_call(
        kernel,
        out_shape=shapes,
        in_specs=[hbm] * 7 + [smem, smem],

        out_specs=(anywhere, anywhere, anywhere),
        scratch_shapes=[
            vmem((16, TOK, FB), BF16),
            vmem((2, 8, TOK, FB), BF16),
            vmem((8, 128), F32),
            vmem((8, 8, 128), F32),
            vmem((2, 8 * TOK, FB), BF16),
            vmem((2, FB, 8 * TOK), BF16),
            vmem((NK, FB, KC), BF16),
            vmem((NK, FB, KC), BF16),
            vmem((2, TOK, KV), BF16),
            vmem((NK, 2 * TOK, KC), F32),
            vmem((NK, NX, 2 * TOK, KC), BF16),
            vmem((NK, NX, 2 * TOK, KC), BF16),
            vmem((NK, 2 * TOK, KC), BF16),
            vmem((NK, 2 * TOK, KC), BF16),
            vmem((NK, 8 * TOK, KC), BF16),
            vmem((NK, FB, KC), F32),
            vmem((NK, FB, KC), BF16),
            vmem((NK, FB, KC), BF16),
            vmem((NK, FB, KC), BF16),
            vmem((64, 128), BF16),
            vmem((64, 128), F32),
            vmem((4, 512, 128), BF16),
            vmem((4, 512, 128), F32),
            vmem((4, 512, 128), BF16),
            vmem((HALF + 16, 128), BF16),
            vmem((HALF + 16, 128), BF16),
            vmem((NZ, PACK, 128), BF16),
            vmem((NZ, PACK, 128), BF16),
            vmem((PACK, 128), F32),
            vmem((PACK, 128), F32),
            vmem((2, NZ * SHARE, 128), BF16),
            vmem((4, 512, 128), BF16),
            vmem((4, 512, 128), BF16),
            dma((34,)),
            dma((14,)), dma((14,)),
            dma((7,)), dma((7,)),
            dma((NK,)), dma((NK,)),
            dma((NK * NX,)), dma((NK * NX,)),
            dma((NK,)), dma((NK,)),
            dma((NK * NX,)), dma((NK * NX,)),
            dma((NK,)), dma((NK,)),
            dma((4,)), dma((4,)),
            dma((NZ,)), dma((NZ,)),
            dma((NZ,)), dma((NZ,)),
            dma((12,)),
        ],
        compiler_params=pltpu.CompilerParams(
            collective_id=0, has_side_effects=True, vmem_limit_bytes=67043328
        ),
        name="window",
    )(
        tokens,
        norm_gain.reshape(64, 128),
        inner_weight,
        cotangent,
        fragment,
        outer_param,
        momentum,
        lag,
        threshold,
    )
    return pl.pallas_call(
        put_out,
        out_shape=shapes,
        in_specs=[anywhere] * 3,
        out_specs=(anywhere,) * 3,
        scratch_shapes=[vmem(shape.shape, BF16) for shape in shapes] + [dma((6,))],
        name="put_out",
    )(*results)


def solution(mesh):
    placed = (
        P("rep", "fsdp", None),
        P(),
        P("rep", "fsdp", None),
        P("rep", "fsdp", None),
        P("rep", "fsdp", None),
        P("fsdp", None),
        P("fsdp", None),
        P("rep"),
        P(),
    )
    return jax.shard_map(
        shards,
        mesh=mesh,
        in_specs=placed,
        out_specs=(P("rep", "fsdp", None), P("rep", "fsdp", None), P("fsdp", None)),
        check_vma=False,
    )
```

```python
import math

import jax
import jax.numpy as jnp
from jax import lax
from jax.experimental import pallas as pl
from jax.experimental.pallas import tpu as pltpu
from jax.sharding import PartitionSpec as P

EPS = 1e-05
MU = 0.9
OUTER_LR = 0.7
ALPHA = 0.5
STARTS = (0.0, 5.0, 10.0, 15.0, 23.0)
STEP = 4.0

NX, NY, NZ = 4, 4, 12
TOK = 128
FB = 512
KV = 512
NK = 2
KC = KV // NK
SHARE = 96
PACK = SHARE + 16
HALF = 1024
F32, BF16 = jnp.float32, jnp.bfloat16
MESH = pl.DeviceIdType.MESH


def kernel(
    tokens, gain, weight, cotangent, fragment, outer, momentum, lag, threshold,
    grad_out, mixed_out, mom_out,
    tokv, tokr, rst_s, rst_r, nrm, nrt, wown, wq, cotv,
    rs_own, rs_s, rs_r, ry_s, ry_r, dk, g_own, g_s, g_r, gout,
    gainv, gainf, fragv, outv, momv, msk, f1r, zs, zr, ys, yr, avg, mixv, momo,
    local_sem, tok_ss, tok_rs, rst_ss, rst_rs, w_ss, w_rs,
    rx_ss, rx_rs, ry_ss, ry_rs, ax_ss, ax_rs, gr_ss, gr_rs,
    f_ss, f_rs, z_ss, z_rs, az_ss, az_rs, out_sem,
):
    rep, fs = lax.axis_index("rep"), lax.axis_index("fsdp")
    core, z, ylo = lax.rem(rep, 2), lax.rem(rep // 2, NZ), rep // (2 * NZ)
    x, y = fs // NY, lax.rem(fs, NY)
    s = 1 - 2 * lax.rem(y + core, 2)
    yp = lax.rem(y + s + NY, NY)
    yq = lax.rem(y - s + NY, NY)
    yo = lax.rem(y + 2, NY)

    def at(i, yy):
        return (rep, lax.rem(x + i + NX, NX) * NY + yy)

    def at_z(i):
        return (ylo * 2 * NZ + lax.rem(z + i, NZ) * 2 + core, fs)

    other_core = (ylo * 2 * NZ + z * 2 + (1 - core), fs)
    other_ylo = ((1 - ylo) * 2 * NZ + z * 2 + core, fs)
    group = [(i, e) for e in (1, 0) for i in (2, 1, 3, 0) if (i, e) != (0, 0)]

    def remote(src, dst, ss, rs, device):
        return pltpu.make_async_remote_copy(
            src_ref=src, dst_ref=dst, send_sem=ss, recv_sem=rs, device_id=device, device_id_type=MESH
        )

    barrier = pltpu.get_barrier_semaphore()
    peers = [at(i, yp if e else y) for i, e in group] + [at(0, yq), other_core, other_ylo]
    peers += [at_z(i) for i in range(1, NZ)]
    for peer in peers:
        pl.semaphore_signal(barrier, inc=1, device_id=peer, device_id_type=MESH)

    tok_in = [
        pltpu.make_async_copy(tokens.at[0, :, pl.ds(b * FB, FB)], tokv.at[b], local_sem.at[b])
        for b in range(NX * NY)
    ]
    w_in = [
        pltpu.make_async_copy(weight.at[0, :, pl.ds(k * KC, KC)], wown.at[k], local_sem.at[16 + k])
        for k in range(NK)
    ]
    frag_in = [
        pltpu.make_async_copy(fragment.at[0, :, pl.ds(c * 128, 128)], fragv.at[c], local_sem.at[20 + c])
        for c in range(4)
    ]
    out_in = [
        pltpu.make_async_copy(outer.at[:, pl.ds(c * 128, 128)], outv.at[c], local_sem.at[24 + c])
        for c in range(4)
    ]
    mom_in = [
        pltpu.make_async_copy(momentum.at[:, pl.ds(c * 128, 128)], momv.at[c], local_sem.at[28 + c])
        for c in range(4)
    ]
    cot_in = pltpu.make_async_copy(cotangent.at[0], cotv.at[0], local_sem.at[32])
    gain_in = pltpu.make_async_copy(gain, gainv, local_sem.at[33])
    loads = tok_in + w_in + frag_in + out_in + [cot_in, gain_in] + mom_in
    for copy in loads:
        copy.start()
    with jax.named_scope("load_wait"):
        for copy in tok_in + w_in:
            copy.wait()
    with jax.named_scope("barrier"):
        pl.semaphore_wait(barrier, len(peers))

    tok_copies = {}
    for n, (i, e) in enumerate(group):
        yd = yp if e else y
        cross = yo if e else yq
        xd = lax.rem(x + i, NX)
        for f, yf in enumerate((yd, cross)):
            copy = remote(
                tokv.at[xd * NY + yf], tokr.at[f, i * 2 + e],
                tok_ss.at[2 * n + f], tok_rs.at[2 * n + f], at(i, yd),
            )
            copy.start()
            tok_copies[i, e, f] = copy
    w_copies = [
        remote(wown.at[k], wq.at[k], w_ss.at[k], w_rs.at[k], at(0, yq)) for k in range(NK)
    ]
    w_copies[0].start()
    cot_in.wait()
    cot_copy = remote(cotv.at[0], cotv.at[1], f_ss.at[3], f_rs.at[3], at(0, yp))

    flag = jnp.where(lag[0] <= threshold[0], 1.0, 0.0).astype(F32)
    for copy in frag_in:
        copy.wait()
    for h in range(2):
        part = fragv[(1 - core) * 2 + h].astype(F32) * flag
        msk[pl.ds(h * 512, 512), :] = part.astype(BF16)
    msk[pl.ds(HALF, 16), :] = jnp.full((16, 128), flag, F32).astype(BF16)
    f1_copy = remote(msk, f1r, f_ss.at[0], f_rs.at[0], other_core)
    f1_copy.start()

    def square(b, total):
        v = tokv[b].astype(F32)
        v = v * v
        return total + (v[:, 0:128] + v[:, 128:256]) + (v[:, 256:384] + v[:, 384:512])

    sums = lax.fori_loop(0, NX * NY, square, jnp.zeros((TOK, 128), F32))
    scale_own = lax.rsqrt(jnp.sum(sums, axis=1, keepdims=True) * (1.0 / (NX * NY * FB)) + EPS)
    rst_s[...] = jnp.broadcast_to(scale_own, (TOK, 128)).T[0:8, :]
    rst_copies = {}
    for n, (i, e) in enumerate(group):
        copy = remote(
            rst_s, rst_r.at[i * 2 + e], rst_ss.at[n], rst_rs.at[n], at(i, yp if e else y)
        )
        copy.start()
        rst_copies[i, e] = copy

    gain_in.wait()
    gainf[...] = gainv[...].astype(F32)
    gains = [
        jnp.concatenate([gainf[pl.ds((x * NY + yy) * 4 + j, 1), :] for j in range(4)], axis=1)
        for yy in (y, yq)
    ]

    def normalise(i, e):
        slot = i * 2 + e
        if slot == 0:
            scale = scale_own
        else:
            rst_copies[i, e].wait_recv()
            scale = jnp.broadcast_to(rst_r[slot, 0:1, :], (TOK, 128)).T[:, 0:1]
        for f in range(2):
            if slot == 0:
                raw = tokv[x * NY + (yq if f else y)]
            else:
                tok_copies[i, e, f].wait_recv()
                raw = tokr[f, slot]
            v = raw.astype(F32) * scale * gains[f]
            nrm[f, pl.ds(slot * TOK, TOK), :] = v.astype(BF16)
            nrt[f, :, pl.ds(slot * TOK, TOK)] = v.T.astype(BF16)

    with jax.named_scope("norm_own"):
        normalise(0, 0)

    with jax.named_scope("f1_wait"):
        f1_copy.wait_recv()
        for copy in out_in:
            copy.wait()
    both = f1r[pl.ds(HALF, 16), :].astype(F32) + flag
    row = both[0:1, :]
    for j in range(NZ):
        for r in range(0, SHARE, 32):
            first = j * SHARE + r
            if first < HALF:
                block, at_row = core * 2 + first // 512, first % 512
                mine = fragv[block, pl.ds(at_row, 32), :].astype(F32) * flag
                theirs = f1r[pl.ds(first, 32), :].astype(F32)
                value = row * outv[block, pl.ds(at_row, 32), :] - (mine + theirs)
            else:
                value = jnp.zeros((32, 128), F32)
            zs[j, pl.ds(r, 32), :] = value.astype(BF16)
        zs[j, pl.ds(SHARE, 16), :] = both.astype(BF16)
    z_copies = [
        remote(zs.at[lax.rem(z + i, NZ)], zr.at[i], z_ss.at[i], z_rs.at[i], at_z(i))
        for i in (6, 5, 7, 4, 8, 3, 9, 2, 10, 1, 11)
    ]
    for copy in z_copies:
        copy.start()

    y_copy = remote(ys, yr, f_ss.at[1], f_rs.at[1], other_ylo)

    def sum_z():
        total = zs[z].astype(F32)
        for copy in z_copies:
            copy.wait_recv()
        for i in range(1, NZ):
            total += zr[i].astype(F32)
        ys[...] = total
        y_copy.start()

    own_share = avg.at[core, pl.ds(pl.multiple_of(z * SHARE, SHARE), SHARE)]
    az_copies = [
        remote(own_share, own_share, az_ss.at[i], az_rs.at[i], at_z(i))
        for i in (6, 5, 7, 4, 8, 3, 9, 2, 10, 1, 11)
    ]
    core_copy = remote(avg.at[core], avg.at[core], f_ss.at[2], f_rs.at[2], other_core)

    def share_average():
        y_copy.wait_recv()
        total = ys[...] + yr[...]
        scale = 1.0 / total[SHARE : SHARE + 1, :]
        own_share[...] = (total[0:SHARE, :] * scale).astype(BF16)
        for copy in az_copies:
            copy.start()

    for i, e in ((1, 0), (3, 0), (2, 0), (0, 1), (1, 1), (3, 1), (2, 1)):
        with jax.named_scope(f"norm_{i}{e}"):
            normalise(i, e)
        if (i, e) == (2, 0):
            with jax.named_scope("sum_z"):
                sum_z()
            w_copies[1].start()
        if (i, e) == (0, 1):
            cot_copy.start()

    rx, ry, ax, gr = {}, {}, {}, {}

    def keys_partial(k):
        w_copies[k].wait_recv()
        for i in (2, 1, 3, 0):
            rows = pl.ds(i * 2 * TOK, 2 * TOK)
            part = jnp.dot(nrm[0, rows, :], wown[k], preferred_element_type=F32)
            part += jnp.dot(nrm[1, rows, :], wq[k], preferred_element_type=F32)
            if i == 0:
                rs_own[k] = part
            else:
                rs_s[k, i] = part.astype(BF16)
                n = k * NX + i
                rx[k, i] = remote(rs_s.at[k, i], rs_r.at[k, i], rx_ss.at[n], rx_rs.at[n], at(-i, y))
                rx[k, i].start()

    def sum_x(k):
        for i in (1, 3, 2):
            rx[k, i].wait_recv()
        total = rs_own[k]
        for i in (1, 2, 3):
            total += rs_r[k, i].astype(F32)
        rs_own[k] = total
        ry_s[k, 0:TOK, :] = total[TOK:, :].astype(BF16)
        ry_s[k, TOK:, :] = total[0:TOK, :].astype(BF16)
        ry[k] = remote(ry_s.at[k], ry_r.at[k], ry_ss.at[k], ry_rs.at[k], at(0, yp))
        ry[k].start()

    def dkeys(k):
        if k == 0:
            cot_copy.wait_recv()
        ry[k].wait_recv()
        keys = rs_own[k] + ry_r[k].astype(F32)
        sig = jax.nn.sigmoid(keys)
        cot = cotv[:, :, pl.ds(k * KC, KC)].astype(F32).reshape(2 * TOK, KC)
        dk[k, 0 : 2 * TOK, :] = (cot * sig * (1.0 + keys * (1.0 - sig))).astype(BF16)
        for i in (2, 1, 3):
            n = k * NX + i
            ax[k, i] = remote(
                dk.at[k, pl.ds(0, 2 * TOK)], dk.at[k, pl.ds(i * 2 * TOK, 2 * TOK)],
                ax_ss.at[n], ax_rs.at[n], at(i, y),
            )
            ax[k, i].start()

    def gradient(k):
        for i in (1, 3, 2):
            ax[k, i].wait_recv()
        g_s[k] = jnp.dot(nrt[1], dk[k], preferred_element_type=F32).astype(BF16)
        gr[k] = remote(g_s.at[k], g_r.at[k], gr_ss.at[k], gr_rs.at[k], at(0, yq))
        gr[k].start()
        g_own[k] = jnp.dot(nrt[0], dk[k], preferred_element_type=F32)

    outs = []

    def finish(k):
        gr[k].wait_recv()
        total = g_own[k] + g_r[k].astype(F32)
        gout[k] = (total * (1.0 / math.sqrt(NX * NY * TOK))).astype(BF16)
        copy = pltpu.make_async_copy(gout.at[k], grad_out.at[0, :, pl.ds(k * KC, KC)], out_sem.at[k])
        copy.start()
        outs.append(copy)

    def gather_average():
        for copy in az_copies:
            copy.wait_recv()
        core_copy.start()

    def outer_update():
        for copy in mom_in:
            copy.wait()
        core_copy.wait_recv()
        for c in range(4):
            average = avg[c // 2, pl.ds(c % 2 * 512, 512), :].astype(F32)
            moment = MU * momv[c].astype(F32) + average
            new_outer = outv[c] - OUTER_LR * (average + MU * moment)
            mixv[c] = (ALPHA * fragv[c].astype(F32) + (1.0 - ALPHA) * new_outer).astype(BF16)
            momo[c] = moment.astype(BF16)
            for buf, out, n in ((mixv, mixed_out.at[0], 4 + c), (momo, mom_out, 8 + c)):
                copy = pltpu.make_async_copy(buf.at[c], out.at[:, pl.ds(c * 128, 128)], out_sem.at[n])
                copy.start()
                outs.append(copy)

    stages = [keys_partial, sum_x, dkeys, gradient, finish]
    steps = [(t + k * STEP, stage, k) for stage, t in zip(stages, STARTS) for k in range(NK)]
    outer_stages = ((share_average, 4.0), (gather_average, 20.0), (outer_update, 22.0))
    steps += [(t, stage, None) for stage, t in outer_stages]
    for _, stage, k in sorted(steps, key=lambda step: step[0]):
        with jax.named_scope(f"{stage.__name__}_{k}"):
            stage() if k is None else stage(k)

    with jax.named_scope("outs"):
        for copy in outs:
            copy.wait()
    sent = list(tok_copies.values()) + w_copies + [f1_copy, y_copy, core_copy, cot_copy]
    sent += list(rst_copies.values()) + z_copies + az_copies
    for group_of in (rx, ry, ax, gr):
        sent += list(group_of.values())
    for copy in sent:
        copy.wait_send()


def put_out(grad, mixed, mom, grad_out, mixed_out, mom_out, g, m, o, sem):
    into = [pltpu.make_async_copy(a, b, sem.at[n]) for n, (a, b) in enumerate(((grad, g), (mixed, m), (mom, o)))]
    out = [
        pltpu.make_async_copy(a, b, sem.at[3 + n])
        for n, (a, b) in enumerate(((g, grad_out), (m, mixed_out), (o, mom_out)))
    ]
    for copy in into:
        copy.start()
    for first, second in zip(into, out):
        first.wait()
        second.start()
    for copy in out:
        copy.wait()


def shards(
    tokens, norm_gain, inner_weight, cotangent, fragment, outer_param, momentum, lag, threshold
):
    vmem, dma = pltpu.VMEM, pltpu.SemaphoreType.DMA
    hbm = pl.BlockSpec(memory_space=pltpu.HBM)
    anywhere = pl.BlockSpec(memory_space=pl.ANY)
    smem = pl.BlockSpec(memory_space=pltpu.SMEM)
    shapes = (
        jax.ShapeDtypeStruct((1, FB, KV), BF16),
        jax.ShapeDtypeStruct((1, FB, KV), BF16),
        jax.ShapeDtypeStruct((FB, KV), BF16),
    )
    results = pl.pallas_call(
        kernel,
        out_shape=shapes,
        in_specs=[hbm] * 7 + [smem, smem],

        out_specs=(anywhere, anywhere, anywhere),
        scratch_shapes=[
            vmem((16, TOK, FB), BF16),
            vmem((2, 8, TOK, FB), BF16),
            vmem((8, 128), F32),
            vmem((8, 8, 128), F32),
            vmem((2, 8 * TOK, FB), BF16),
            vmem((2, FB, 8 * TOK), BF16),
            vmem((NK, FB, KC), BF16),
            vmem((NK, FB, KC), BF16),
            vmem((2, TOK, KV), BF16),
            vmem((NK, 2 * TOK, KC), F32),
            vmem((NK, NX, 2 * TOK, KC), BF16),
            vmem((NK, NX, 2 * TOK, KC), BF16),
            vmem((NK, 2 * TOK, KC), BF16),
            vmem((NK, 2 * TOK, KC), BF16),
            vmem((NK, 8 * TOK, KC), BF16),
            vmem((NK, FB, KC), F32),
            vmem((NK, FB, KC), BF16),
            vmem((NK, FB, KC), BF16),
            vmem((NK, FB, KC), BF16),
            vmem((64, 128), BF16),
            vmem((64, 128), F32),
            vmem((4, 512, 128), BF16),
            vmem((4, 512, 128), F32),
            vmem((4, 512, 128), BF16),
            vmem((HALF + 16, 128), BF16),
            vmem((HALF + 16, 128), BF16),
            vmem((NZ, PACK, 128), BF16),
            vmem((NZ, PACK, 128), BF16),
            vmem((PACK, 128), F32),
            vmem((PACK, 128), F32),
            vmem((2, NZ * SHARE, 128), BF16),
            vmem((4, 512, 128), BF16),
            vmem((4, 512, 128), BF16),
            dma((34,)),
            dma((14,)), dma((14,)),
            dma((7,)), dma((7,)),
            dma((NK,)), dma((NK,)),
            dma((NK * NX,)), dma((NK * NX,)),
            dma((NK,)), dma((NK,)),
            dma((NK * NX,)), dma((NK * NX,)),
            dma((NK,)), dma((NK,)),
            dma((4,)), dma((4,)),
            dma((NZ,)), dma((NZ,)),
            dma((NZ,)), dma((NZ,)),
            dma((12,)),
        ],
        compiler_params=pltpu.CompilerParams(
            collective_id=0, has_side_effects=True, vmem_limit_bytes=67043328
        ),
        name="window",
    )(
        tokens,
        norm_gain.reshape(64, 128),
        inner_weight,
        cotangent,
        fragment,
        outer_param,
        momentum,
        lag,
        threshold,
    )
    return pl.pallas_call(
        put_out,
        out_shape=shapes,
        in_specs=[anywhere] * 3,
        out_specs=(anywhere,) * 3,
        scratch_shapes=[vmem(shape.shape, BF16) for shape in shapes] + [dma((6,))],
        name="put_out",
    )(*results)


def solution(mesh):
    placed = (
        P("rep", "fsdp", None),
        P(),
        P("rep", "fsdp", None),
        P("rep", "fsdp", None),
        P("rep", "fsdp", None),
        P("fsdp", None),
        P("fsdp", None),
        P("rep"),
        P(),
    )
    return jax.shard_map(
        shards,
        mesh=mesh,
        in_specs=placed,
        out_specs=(P("rep", "fsdp", None), P("rep", "fsdp", None), P("fsdp", None)),
        check_vma=False,
    )
```
